768 devices in a mesh: grp: 96 (over x, y_lo, z), sub: 8 (over y_hi, core).
Axes of the slice: x: 4, y: 8 (y_hi: 4, y_lo: 2; y = y_hi * 2 + y_lo), z: 12, core: 2. Of those that a mesh axis runs over, the one named last changes fastest.
Arguments:
- residual: float32 [2359296], P(('grp', 'sub')), may hold values from -6 to 6
- edge_scale: float32 [2359296], P(('grp', 'sub')), may hold values from 0.2 to 1
- tangent: float32 [3, 2359296], P(None, ('grp', 'sub')), may hold values from -6 to 6
- edge_tail: int32 [2359296], P(('grp', 'sub')), may hold values from 0 to 511
- edge_head: int32 [2359296], P(('grp', 'sub')), may hold values from 0 to 4607
- stencil_index: int32 [14, 393216], P(None, ('grp', 'sub')), may hold values from 0 to 4607
- stencil_coef: bfloat16 [4, 14, 393216], P(None, None, ('grp', 'sub')), may hold values from -1 to -0.099609375
- diag_margin: float32 [4, 393216], P(None, ('grp', 'sub')), may hold values from 0.05 to 0.5
- send_index: int32 [192, 16, 512], P('grp', 'sub'), may hold values from 0 to 511
Outputs:
- correction: float32 [2359296], P(('grp', 'sub'))
The draws below stay inside these ranges and needn't reach their ends.
Inputs may be any that keep to these rules, and one draw needn't show every extreme that they name: `edge_tail`: positions among a device's own nodes. `edge_head`: positions in the device's extended list: own nodes first, then the 8 received blocks. `stencil_index`: positions in the extended list of the device that holds the row. `send_index`: positions among the device's own nodes; an entry may repeat.
All inputs are finite; a program needn't handle non-finite values.
Results may differ from the reference program's by a relative error of at most 0.0003.
Values sent between devices are 32-bit elements; how exact they have to be, the bound alone decides.
No kernel may reach another device: no remote copies, remote signals or barrier semaphores. Data moves between devices by JAX's collectives and lax.ppermute only.
A program may use at most 32 MiB of HBM per device.

```python
import math
import jax
import jax.numpy as jnp

N_DEV = 512
E_DEV = 3072
HALO = 512
STENCIL = 14
SWEEPS = 4
NODES = 393216
EDGES = 2359296
N_GRP = 96
N_SUB = 8


def with_ends(entries, stream_key, smallest, top_value):
    longest = entries.shape.index(max(entries.shape))
    spots = []
    for shift in (0, 1):
        where = [jax.random.randint(jax.random.fold_in(stream_key, axis), (), 0, length) for axis, length in enumerate(entries.shape)]
        where[longest] = (where[longest] + shift) % entries.shape[longest]
        spots.append(tuple(where))
    return entries.at[spots[0]].set(smallest).at[spots[1]].set(top_value)


def steps_of(stream_key, extent, pieces, smallest, largest):
    factor_of, own = 1.0, jax.random.fold_in(stream_key, 6)
    for dim, shards_of in pieces:
        draws = jnp.exp(jax.random.uniform(jax.random.fold_in(own, dim), (shards_of,), jnp.float32, smallest / len(pieces), largest / len(pieces)))
        factor_of = factor_of * jnp.repeat(draws, extent[dim] // shards_of).reshape([-1 if axis == dim else 1 for axis in range(len(extent))])
    return factor_of


def scatter_about(key, shape, scale, bound, cuts=(), kind=jnp.bfloat16):
    drawn = jax.random.normal(key, shape, jnp.float32) * scale
    if len(cuts) > 0:
        drawn = steps_of(key, shape, cuts, -0.22, 0.18) * drawn
    return jnp.clip(drawn, min=-bound, max=bound).astype(kind)


def setup_inputs(seed: int = 0) -> dict:
    arg_keys = jax.random.split(jax.random.key(seed), 10)
    return {
        "residual": scatter_about(arg_keys[0], (EDGES,), 1.0, 6.0, ((0, 768),), jnp.float32),
        "edge_scale": jnp.clip(jnp.exp(math.log(1.0) - 1.609438 * jax.random.uniform(arg_keys[1], (EDGES,), jnp.float32) ** steps_of(arg_keys[1], (EDGES,), ((0, 768),), -0.2, 0.2)), 0.2, 1.0),
        "tangent": scatter_about(arg_keys[2], (3, EDGES), 1.0, 6.0, ((1, 768),), jnp.float32),
        "edge_tail": with_ends(jax.random.randint(arg_keys[3], (EDGES,), 0, N_DEV), jax.random.fold_in(arg_keys[3], 1), 0, N_DEV - 1).astype(jnp.int32),
        "edge_head": with_ends(jax.random.randint(arg_keys[4], (EDGES,), 0, N_DEV + 8 * HALO), jax.random.fold_in(arg_keys[4], 1), 0, (N_DEV + 8 * HALO) - 1).astype(jnp.int32),
        "stencil_index": with_ends(jax.random.randint(arg_keys[5], (STENCIL, NODES), 0, N_DEV + 8 * HALO), jax.random.fold_in(arg_keys[5], 1), 0, (N_DEV + 8 * HALO) - 1).astype(jnp.int32),
        "stencil_coef": jnp.clip(-1.0 + 0.9003906 * jax.random.uniform(arg_keys[6], (4, STENCIL, NODES), jnp.float32) ** steps_of(arg_keys[6], (4, STENCIL, NODES), ((2, 768),), -0.2, 0.2), -1.0, -0.099609375).astype(jnp.bfloat16),
        "diag_margin": jnp.clip(jnp.exp(math.log(0.5) - 2.3025851 * jax.random.uniform(arg_keys[7], (4, NODES), jnp.float32) ** steps_of(arg_keys[7], (4, NODES), ((1, 768),), -0.2, 0.2)), 0.05, 0.5),
        "send_index": with_ends(jax.random.randint(arg_keys[8], (2 * N_GRP, 2 * N_SUB, HALO), 0, N_DEV), jax.random.fold_in(arg_keys[8], 1), 0, N_DEV - 1).astype(jnp.int32),
    }


def ghost_table(send_index):
    blocks = send_index.reshape(N_GRP, 2, N_SUB, 2, HALO).transpose(0, 2, 1, 3, 4)
    owner_base = (jnp.arange(N_GRP * N_SUB, dtype=jnp.int32) * N_DEV).reshape(N_GRP, N_SUB, 1, 1, 1)
    global_ids = blocks + owner_base
    from_below = jnp.roll(global_ids, 1, axis=0)[:, :, 1]
    from_above = jnp.roll(global_ids, -1, axis=0)[:, :, 0]
    from_prev = jnp.roll(global_ids, 1, axis=1)[:, :, :, 1]
    from_next = jnp.roll(global_ids, -1, axis=1)[:, :, :, 0]
    ghosts = jnp.concatenate([from_below, from_above, from_prev, from_next], axis=2)
    ghosts = ghosts.reshape(N_GRP * N_SUB, 8 * HALO)
    own_ids = jnp.arange(N_GRP * N_SUB * N_DEV, dtype=jnp.int32).reshape(N_GRP * N_SUB, N_DEV)
    return jnp.concatenate([own_ids, ghosts], axis=1).reshape(-1)


def to_global(flat_table, local, per_device):
    extended = N_DEV + 8 * HALO
    device = (jnp.arange(local.shape[-1], dtype=jnp.int32) // per_device).astype(jnp.int32)
    return flat_table[device * extended + local.astype(jnp.int32)]


def reference(residual, edge_scale, tangent, edge_tail, edge_head, stencil_index, stencil_coef, diag_margin, send_index):
    flat_table = ghost_table(send_index)
    tail_ids = to_global(flat_table, edge_tail, E_DEV)
    head_ids = to_global(flat_table, edge_head, E_DEV)
    node_total = N_DEV * N_GRP * N_SUB
    half_terms = 0.5 * tangent * residual[None, :]
    vals_tail = jnp.concatenate([-residual[None, :], half_terms], axis=0)
    vals_head = jnp.concatenate([residual[None, :], half_terms], axis=0)
    node_sums = jnp.zeros((4, node_total), jnp.float32)
    node_sums = node_sums.at[:, tail_ids].add(vals_tail).at[:, head_ids].add(vals_head)
    neighbour_ids = [to_global(flat_table, stencil_index[column], N_DEV) for column in range(STENCIL)]
    diag_vals = jnp.zeros((4, node_total), jnp.float32)
    for column in range(STENCIL):
        diag_vals = diag_vals + jnp.abs(stencil_coef[:, column].astype(jnp.float32))
    diag_vals = (1.0 + diag_margin) * diag_vals
    solved = node_sums / diag_vals
    for sweep in range(SWEEPS - 1):
        applied = diag_vals * solved
        for column in range(STENCIL):
            applied = applied + stencil_coef[:, column].astype(jnp.float32) * solved[:, neighbour_ids[column]]
        solved = solved + (node_sums - applied) / diag_vals
    at_tail = solved[:, tail_ids]
    at_head = solved[:, head_ids]
    return edge_scale * residual + (at_head[0] - at_tail[0]) + 0.5 * jnp.sum(tangent * (at_tail[1:] + at_head[1:]), axis=0)
```

```python
import jax
import jax.numpy as jnp
from jax import lax
from jax.experimental import pallas as pl
from jax.experimental.pallas import tpu as pltpu
from jax.sharding import PartitionSpec as P

SWEEPS = 4
LANES = 128
F32 = jnp.float32
BF16 = jnp.bfloat16
VMEM = pl.BlockSpec(memory_space=pltpu.VMEM)
SMEM = pl.BlockSpec(memory_space=pltpu.SMEM)


def call(kernel, outs, *args, flops=1 << 20):
    return pl.pallas_call(
        kernel,
        out_shape=[jax.ShapeDtypeStruct(shape, dtype) for shape, dtype in outs],
        in_specs=[SMEM] + [VMEM] * (len(args) - 1),
        out_specs=[VMEM] * len(outs),
    )(*args)


def pairs(size, offset):
    route = []
    for k in range(size // 2):
        low, high = (2 * k + offset) % size, (2 * k + 1 + offset) % size
        route += [(low, high), (high, low)]
    return route


def split3(value):
    first = value.astype(BF16).astype(F32)
    rest = value - first
    second = rest.astype(BF16).astype(F32)
    third = (rest - second).astype(BF16).astype(F32)
    return (first, second, third)


def nt_dot(left, right):
    return lax.dot_general(left, right, (((1,), (1,)), ((), ())), preferred_element_type=F32)


def lane_pick(row, lane):
    wide = jnp.broadcast_to(row, lane.shape)
    return jnp.take_along_axis(wide, lane, axis=1, mode="promise_in_bounds")


def rows_of(index):
    return lax.shift_right_logical(index, 7), jnp.bitwise_and(index, LANES - 1)


def onehot(lane):
    n = lane.shape[1]
    iota = lax.broadcasted_iota(jnp.int32, (LANES, n), 0)
    return jnp.where(iota == lane, 1.0, 0.0).astype(BF16)


def masked(values, row, count):
    iota = lax.broadcasted_iota(jnp.int32, (count, row.shape[1]), 0)
    mask = iota == row
    return jnp.concatenate([jnp.where(mask, v, 0.0) for v in values], axis=0).astype(BF16)


def sides(par, odd, even):
    low = jnp.where(par == 1, even, odd)
    high = jnp.where(par == 1, odd, even)
    return low, high


def edge_sums(par, res_ref, tan_ref, tail_ref, head_ref, own_ref, og_ref, eg_ref, os_ref, es_ref):
    edges = res_ref.shape[1]
    chunk = 512
    total_head, total_tail = None, None
    for start in range(0, edges, chunk):
        cut = slice(start, start + chunk)
        res = res_ref[:, cut]
        half = [0.5 * tan_ref[c : c + 1, cut] * res for c in range(3)]
        head_row, head_lane = rows_of(head_ref[:, cut])
        head_row = jnp.where(head_row >= 4, head_row + 4, head_row)
        tail_row, tail_lane = rows_of(tail_ref[:, cut])
        parts = [split3(v) for v in [res] + half]
        parts = [parts[c][p] for p in range(3) for c in range(4)]
        signed = [-v if i % 4 == 0 else v for i, v in enumerate(parts)]
        by_head = nt_dot(masked(parts, head_row, 40), onehot(head_lane))
        by_tail = nt_dot(masked(signed, tail_row, 8), onehot(tail_lane))
        total_head = by_head if total_head is None else total_head + by_head
        total_tail = by_tail if total_tail is None else total_tail + by_tail
    g_odd, s_odd = par[0], par[1]
    for c in range(4):
        head = total_head[40 * c : 40 * c + 40]
        tail = total_tail[8 * c : 8 * c + 8]
        for p in (1, 2):
            at = 4 * p + c
            head = head + total_head[40 * at : 40 * at + 40]
            tail = tail + total_tail[8 * at : 8 * at + 8]
        own_ref[4 * c : 4 * c + 4, :] = head[0:4] + tail[0:4]
        before, after, prev, nxt = (head[8 * i : 8 * i + 8] for i in range(1, 5))
        og_ref[c] = jnp.where(g_odd == 1, after, before)
        eg_ref[c] = jnp.where(g_odd == 1, before, after)
        os_ref[c] = jnp.where(s_odd == 1, nxt, prev)
        es_ref[c] = jnp.where(s_odd == 1, prev, nxt)


def prepare(par, idx_ref, coef_ref, margin_ref, send_ref, idx16_ref, coef16_ref, dinv_ref, send16_ref):
    count = idx_ref.shape[0]
    idx16_ref[0:count, :] = idx_ref[...]
    idx16_ref[count:16, :] = jnp.zeros((16 - count, idx_ref.shape[1]), jnp.int32)
    for k in range(4):
        wide = coef_ref[k].astype(F32)
        coef16_ref[k, 0:count, :] = wide
        coef16_ref[k, count:16, :] = jnp.zeros((16 - count, wide.shape[1]), F32)
        diag = (1.0 + margin_ref[k : k + 1, :]) * jnp.sum(jnp.abs(wide), axis=0, keepdims=True)
        inverse = 1.0 / diag
        for q in range(4):
            dinv_ref[4 * k + q : 4 * k + q + 1, :] = inverse[:, LANES * q : LANES * q + LANES]
    for a in range(2):
        for b in range(2):
            for q in range(4):
                at = 8 * a + 4 * b + q
                send16_ref[at : at + 1, :] = send_ref[a, b : b + 1, LANES * q : LANES * q + LANES]


def send_blocks(par, solved, send_ref, outs):
    g_odd, s_odd = par[0], par[1]
    og_ref, eg_ref, os_ref, es_ref = outs
    row, lane = rows_of(send_ref[...])
    for k in range(4):
        low, high = None, None
        got = []
        for half in range(2):
            part = slice(8 * half, 8 * half + 8)
            acc = lane_pick(solved[4 * k : 4 * k + 1], lane[part])
            for r in range(1, 4):
                acc = jnp.where(row[part] == r, lane_pick(solved[4 * k + r : 4 * k + r + 1], lane[part]), acc)
            got.append(acc)
        low, high = got
        og_ref[k] = jnp.where(g_odd == 1, high, low)
        eg_ref[k] = jnp.where(g_odd == 1, low, high)
        left = jnp.concatenate([low[0:4], high[0:4]], axis=0)
        right = jnp.concatenate([low[4:8], high[4:8]], axis=0)
        os_ref[k] = jnp.where(s_odd == 1, right, left)
        es_ref[k] = jnp.where(s_odd == 1, left, right)


def first_solve(par, own_ref, og, eg, os, es, send_ref, dinv_ref, rn_ref, y_ref, *outs):
    index = send_ref[...]
    row, lane = rows_of(index)
    lefts, rights = [], []
    values = []
    for c in range(4):
        before, after = sides(par[0], og[c], eg[c])
        prev, nxt = sides(par[1], os[c], es[c])
        low = before + jnp.concatenate([prev[0:4], nxt[0:4]], axis=0)
        high = after + jnp.concatenate([prev[4:8], nxt[4:8]], axis=0)
        values.append([split3(low), split3(high)])
    for half in range(2):
        for i in range(8):
            at = 8 * half + i
            cut = [values[c][half][p][i : i + 1] for p in range(3) for c in range(4)]
            lefts.append(masked(cut, row[at : at + 1], 8))
            rights.append(onehot(lane[at : at + 1]))
    total = nt_dot(jnp.concatenate(lefts, axis=1), jnp.concatenate(rights, axis=1))
    rows = []
    for c in range(4):
        rows.append(sum(total[8 * (4 * p + c) : 8 * (4 * p + c) + 4] for p in range(3)))
    rn = own_ref[...] + jnp.concatenate(rows, axis=0)
    solved = rn * dinv_ref[...]
    rn_ref[...] = rn
    y_ref[...] = solved
    send_blocks(par, solved, send_ref, outs)


def tables(par, y, og, eg, os, es):
    result = []
    for k in range(4):
        before, after = sides(par[0], og[k], eg[k])
        prev, nxt = sides(par[1], os[k], es[k])
        blocks = [y[4 * k : 4 * k + 4], before, after, prev, nxt]
        result.append([block[r : r + 1] for block in blocks for r in range(block.shape[0])])
    return result


def gathered(table, index):
    rows, lanes = zip(*(rows_of(i) for i in index))
    acc = [[None] * 4 for _ in index]
    for r in range(len(table[0])):
        for v in range(len(index)):
            mask = rows[v] == r
            for k in range(4):
                got = lane_pick(table[k][r], lanes[v])
                acc[v][k] = got if r == 0 else jnp.where(mask, got, acc[v][k])
    return acc


def sweep(par, y_ref, og, eg, os, es, idx_ref, coef_ref, rn_ref, dinv_ref, send_ref, new_ref, *outs):
    table = tables(par, y_ref[...], og, eg, os, es)
    index = [idx_ref[8 * u : 8 * u + 8, LANES * q : LANES * q + LANES] for q in range(4) for u in range(2)]
    got = gathered(table, index)
    rows = []
    for k in range(4):
        for q in range(4):
            cols = slice(LANES * q, LANES * q + LANES)
            total = got[2 * q][k] * coef_ref[k, 0:8, cols] + got[2 * q + 1][k] * coef_ref[k, 8:16, cols]
            rows.append(jnp.sum(total, axis=0, keepdims=True))
    solved = (rn_ref[...] - jnp.concatenate(rows, axis=0)) * dinv_ref[...]
    new_ref[...] = solved
    send_blocks(par, solved, send_ref, outs)


def edge_values(par, y_ref, og, eg, os, es, res_ref, scale_ref, tan_ref, tail_ref, head_ref, out_ref):
    table = tables(par, y_ref[...], og, eg, os, es)
    groups = res_ref.shape[0] // 8
    heads = gathered(table, [head_ref[8 * v : 8 * v + 8] for v in range(groups)])
    tails = gathered([t[:4] for t in table], [tail_ref[8 * v : 8 * v + 8] for v in range(groups)])
    for v in range(groups):
        part = slice(8 * v, 8 * v + 8)
        total = scale_ref[part] * res_ref[part] + (heads[v][0] - tails[v][0])
        mixed = None
        for c in range(3):
            pieces = [tan_ref[c : c + 1, LANES * i : LANES * i + LANES] for i in range(8 * v, 8 * v + 8)]
            term = jnp.concatenate(pieces, axis=0) * (tails[v][c + 1] + heads[v][c + 1])
            mixed = term if mixed is None else mixed + term
        out_ref[part] = total + 0.5 * mixed


def exchange(blocks):
    og, eg, os, es = blocks
    grp, sub = lax.axis_size("grp"), lax.axis_size("sub")
    og = lax.ppermute(og, "grp", pairs(grp, 1))
    eg = lax.ppermute(eg, "grp", pairs(grp, 0))
    os = lax.ppermute(os, "sub", pairs(sub, 1))
    es = lax.ppermute(es, "sub", pairs(sub, 0))
    return og, eg, os, es


def body(
    residual,
    edge_scale,
    tangent,
    edge_tail,
    edge_head,
    stencil_index,
    stencil_coef,
    diag_margin,
    send_index,
):
    nodes = diag_margin.shape[1]
    par = jnp.stack([lax.axis_index("grp") % 2, lax.axis_index("sub") % 2]).astype(jnp.int32)
    own = ((16, LANES), F32)
    block = [((4, 8, LANES), F32)] * 4
    flat = lambda x: x.reshape(1, -1)
    tile = lambda x: x.reshape(-1, LANES)

    partial, *ghost = call(edge_sums, [own] + block, par, flat(residual), tangent, flat(edge_tail), flat(edge_head))
    idx16, coef16, dinv, send16 = call(
        prepare,
        [((16, nodes), jnp.int32), ((4, 16, nodes), F32), own, ((16, LANES), jnp.int32)],
        par, stencil_index, stencil_coef, diag_margin, send_index,
    )
    ghost = exchange(ghost)
    rn, solved, *blocks = call(first_solve, [own, own] + block, par, partial, *ghost, send16, dinv)
    for _ in range(SWEEPS - 1):
        blocks = exchange(blocks)
        solved, *blocks = call(
            sweep, [own] + block, par, solved, *blocks, idx16, coef16, rn, dinv, send16
        )
    blocks = exchange(blocks)
    (out,) = call(
        edge_values,
        [((residual.shape[0] // LANES, LANES), F32)],
        par, solved, *blocks, tile(residual), tile(edge_scale), tangent, tile(edge_tail), tile(edge_head),
    )
    return out.reshape(-1)


def solution(mesh):
    return jax.shard_map(
        body,
        mesh=mesh,
        in_specs=(
            P(("grp", "sub")),
            P(("grp", "sub")),
            P(None, ("grp", "sub")),
            P(("grp", "sub")),
            P(("grp", "sub")),
            P(None, ("grp", "sub")),
            P(None, None, ("grp", "sub")),
            P(None, ("grp", "sub")),
            P("grp", "sub", None),
        ),
        out_specs=P(("grp", "sub")),
        check_vma=False,
    )
```

```python
import jax
import jax.numpy as jnp
from jax import lax
from jax.experimental import pallas as pl
from jax.experimental.pallas import tpu as pltpu
from jax.sharding import PartitionSpec as P

SWEEPS = 4
LANES = 128
F32 = jnp.float32
BF16 = jnp.bfloat16
VMEM = pl.BlockSpec(memory_space=pltpu.VMEM)


def call(kernel, outs, *args):
    return pl.pallas_call(
        kernel,
        out_shape=[jax.ShapeDtypeStruct(shape, dtype) for shape, dtype in outs],
        in_specs=[VMEM] * len(args),
        out_specs=[VMEM] * len(outs),
        compiler_params=pltpu.CompilerParams(vmem_limit_bytes=16 << 20),
    )(*args)


def pairs(size, offset):
    route = []
    for k in range(size // 2):
        low, high = (2 * k + offset) % size, (2 * k + 1 + offset) % size
        route += [(low, high), (high, low)]
    return route


def split3(value):
    first = value.astype(BF16).astype(F32)
    rest = value - first
    second = rest.astype(BF16).astype(F32)
    third = (rest - second).astype(BF16).astype(F32)
    return (first, second, third)


def nt_dot(left, right):
    return lax.dot_general(left, right, (((1,), (1,)), ((), ())), preferred_element_type=F32)


def lane_pick(row, lane):
    wide = jnp.broadcast_to(row, lane.shape)
    return jnp.take_along_axis(wide, lane, axis=1, mode="promise_in_bounds")


def rows_of(index):
    return lax.shift_right_logical(index, 7), jnp.bitwise_and(index, LANES - 1)


def onehot(lane):
    n = lane.shape[1]
    iota = lax.broadcasted_iota(jnp.int32, (LANES, n), 0)
    return jnp.where(iota == lane, 1.0, 0.0).astype(BF16)


def masked(values, row, count):
    iota = lax.broadcasted_iota(jnp.int32, (count, row.shape[1]), 0)
    mask = iota == row
    return jnp.concatenate([jnp.where(mask, v, 0.0) for v in values], axis=0).astype(BF16)


def odd(axis):
    return jnp.bitwise_and(lax.axis_index(axis), 1)


def sides(parity, by_odd, by_even):
    low = jnp.where(parity == 1, by_even, by_odd)
    high = jnp.where(parity == 1, by_odd, by_even)
    return low, high


def edge_sums(res_ref, tan_ref, tail_ref, head_ref, own_ref, og_ref, eg_ref, os_ref, es_ref):
    edges = res_ref.shape[1]
    chunk = 512
    total_head, total_tail = None, None
    for start in range(0, edges, chunk):
        cut = slice(start, start + chunk)
        res = res_ref[:, cut]
        half = [0.5 * tan_ref[c : c + 1, cut] * res for c in range(3)]
        head_row, head_lane = rows_of(head_ref[:, cut])
        head_row = jnp.where(head_row >= 4, head_row + 4, head_row)
        tail_row, tail_lane = rows_of(tail_ref[:, cut])
        parts = [split3(v) for v in [res] + half]
        parts = [parts[c][p] for p in range(3) for c in range(4)]
        signed = [-v if i % 4 == 0 else v for i, v in enumerate(parts)]
        by_head = nt_dot(masked(parts, head_row, 40), onehot(head_lane))
        by_tail = nt_dot(masked(signed, tail_row, 8), onehot(tail_lane))
        total_head = by_head if total_head is None else total_head + by_head
        total_tail = by_tail if total_tail is None else total_tail + by_tail
    g_odd, s_odd = odd("grp"), odd("sub")
    for c in range(4):
        head = total_head[40 * c : 40 * c + 40]
        tail = total_tail[8 * c : 8 * c + 8]
        for p in (1, 2):
            at = 4 * p + c
            head = head + total_head[40 * at : 40 * at + 40]
            tail = tail + total_tail[8 * at : 8 * at + 8]
        own_ref[4 * c : 4 * c + 4, :] = head[0:4] + tail[0:4]
        before, after, prev, nxt = (head[8 * i : 8 * i + 8] for i in range(1, 5))
        og_ref[c] = jnp.where(g_odd == 1, after, before)
        eg_ref[c] = jnp.where(g_odd == 1, before, after)
        os_ref[c] = jnp.where(s_odd == 1, nxt, prev)
        es_ref[c] = jnp.where(s_odd == 1, prev, nxt)


def prepare(idx_ref, coef_ref, margin_ref, send_ref, idx16_ref, coef16_ref, dinv_ref, send16_ref):
    count = idx_ref.shape[0]
    idx16_ref[0:count, :] = idx_ref[...]
    idx16_ref[count:16, :] = jnp.zeros((16 - count, idx_ref.shape[1]), jnp.int32)
    for k in range(4):
        wide = coef_ref[k].astype(F32)
        coef16_ref[k, 0:count, :] = wide
        coef16_ref[k, count:16, :] = jnp.zeros((16 - count, wide.shape[1]), F32)
        diag = (1.0 + margin_ref[k : k + 1, :]) * jnp.sum(jnp.abs(wide), axis=0, keepdims=True)
        inverse = 1.0 / diag
        for q in range(4):
            dinv_ref[4 * k + q : 4 * k + q + 1, :] = inverse[:, LANES * q : LANES * q + LANES]
    for a in range(2):
        for b in range(2):
            for q in range(4):
                at = 8 * a + 4 * b + q
                send16_ref[at : at + 1, :] = send_ref[a, b : b + 1, LANES * q : LANES * q + LANES]


def send_blocks(solved, send_ref, outs):
    g_odd, s_odd = odd("grp"), odd("sub")
    og_ref, eg_ref, os_ref, es_ref = outs
    row, lane = rows_of(send_ref[...])
    for k in range(4):
        low, high = None, None
        got = []
        for half in range(2):
            part = slice(8 * half, 8 * half + 8)
            acc = lane_pick(solved[4 * k : 4 * k + 1], lane[part])
            for r in range(1, 4):
                acc = jnp.where(row[part] == r, lane_pick(solved[4 * k + r : 4 * k + r + 1], lane[part]), acc)
            got.append(acc)
        low, high = got
        og_ref[k] = jnp.where(g_odd == 1, high, low)
        eg_ref[k] = jnp.where(g_odd == 1, low, high)
        left = jnp.concatenate([low[0:4], high[0:4]], axis=0)
        right = jnp.concatenate([low[4:8], high[4:8]], axis=0)
        os_ref[k] = jnp.where(s_odd == 1, right, left)
        es_ref[k] = jnp.where(s_odd == 1, left, right)


def first_solve(own_ref, og, eg, os, es, send_ref, dinv_ref, rn_ref, y_ref, *outs):
    index = send_ref[...]
    row, lane = rows_of(index)
    lefts, rights = [], []
    values = []
    for c in range(4):
        before, after = sides(odd("grp"), og[c], eg[c])
        prev, nxt = sides(odd("sub"), os[c], es[c])
        low = before + jnp.concatenate([prev[0:4], nxt[0:4]], axis=0)
        high = after + jnp.concatenate([prev[4:8], nxt[4:8]], axis=0)
        values.append([split3(low), split3(high)])
    for half in range(2):
        for i in range(8):
            at = 8 * half + i
            cut = [values[c][half][p][i : i + 1] for p in range(3) for c in range(4)]
            lefts.append(masked(cut, row[at : at + 1], 8))
            rights.append(onehot(lane[at : at + 1]))
    total = nt_dot(jnp.concatenate(lefts, axis=1), jnp.concatenate(rights, axis=1))
    rows = []
    for c in range(4):
        rows.append(sum(total[8 * (4 * p + c) : 8 * (4 * p + c) + 4] for p in range(3)))
    rn = own_ref[...] + jnp.concatenate(rows, axis=0)
    solved = rn * dinv_ref[...]
    rn_ref[...] = rn
    y_ref[...] = solved
    send_blocks(solved, send_ref, outs)


def tables(y, og, eg, os, es):
    result = []
    for k in range(4):
        before, after = sides(odd("grp"), og[k], eg[k])
        prev, nxt = sides(odd("sub"), os[k], es[k])
        blocks = [y[4 * k : 4 * k + 4], before, after, prev, nxt]
        result.append([block[r : r + 1] for block in blocks for r in range(block.shape[0])])
    return result


def gathered(table, index):
    rows, lanes = zip(*(rows_of(i) for i in index))
    acc = [[None] * 4 for _ in index]
    for r in range(len(table[0])):
        for v in range(len(index)):
            mask = rows[v] == r
            for k in range(4):
                got = lane_pick(table[k][r], lanes[v])
                acc[v][k] = got if r == 0 else jnp.where(mask, got, acc[v][k])
    return acc


def sweep(y_ref, og, eg, os, es, idx_ref, coef_ref, rn_ref, dinv_ref, send_ref, new_ref, *outs):
    table = tables(y_ref[...], og, eg, os, es)
    index = [idx_ref[8 * u : 8 * u + 8, LANES * q : LANES * q + LANES] for q in range(4) for u in range(2)]
    got = gathered(table, index)
    rows = []
    for k in range(4):
        for q in range(4):
            cols = slice(LANES * q, LANES * q + LANES)
            total = got[2 * q][k] * coef_ref[k, 0:8, cols] + got[2 * q + 1][k] * coef_ref[k, 8:16, cols]
            rows.append(jnp.sum(total, axis=0, keepdims=True))
    solved = (rn_ref[...] - jnp.concatenate(rows, axis=0)) * dinv_ref[...]
    new_ref[...] = solved
    send_blocks(solved, send_ref, outs)


def edge_values(y_ref, og, eg, os, es, res_ref, scale_ref, tan_ref, tail_ref, head_ref, out_ref):
    table = tables(y_ref[...], og, eg, os, es)
    groups = res_ref.shape[0] // 8
    heads = gathered(table, [head_ref[8 * v : 8 * v + 8] for v in range(groups)])
    tails = gathered([t[:4] for t in table], [tail_ref[8 * v : 8 * v + 8] for v in range(groups)])
    for v in range(groups):
        part = slice(8 * v, 8 * v + 8)
        total = scale_ref[part] * res_ref[part] + (heads[v][0] - tails[v][0])
        mixed = None
        for c in range(3):
            pieces = [tan_ref[c : c + 1, LANES * i : LANES * i + LANES] for i in range(8 * v, 8 * v + 8)]
            term = jnp.concatenate(pieces, axis=0) * (tails[v][c + 1] + heads[v][c + 1])
            mixed = term if mixed is None else mixed + term
        out_ref[part] = total + 0.5 * mixed


def exchange(blocks):
    og, eg, os, es = blocks
    grp, sub = lax.axis_size("grp"), lax.axis_size("sub")
    og = lax.ppermute(og, "grp", pairs(grp, 1))
    eg = lax.ppermute(eg, "grp", pairs(grp, 0))
    os = lax.ppermute(os, "sub", pairs(sub, 1))
    es = lax.ppermute(es, "sub", pairs(sub, 0))
    return og, eg, os, es


def body(
    residual,
    edge_scale,
    tangent,
    edge_tail,
    edge_head,
    stencil_index,
    stencil_coef,
    diag_margin,
    send_index,
):
    nodes = diag_margin.shape[1]
    own = ((16, LANES), F32)
    block = [((4, 8, LANES), F32)] * 4
    flat = lambda x: x.reshape(1, -1)
    tile = lambda x: x.reshape(-1, LANES)

    partial, *ghost = call(edge_sums, [own] + block, flat(residual), tangent, flat(edge_tail), flat(edge_head))
    idx16, coef16, dinv, send16 = call(
        prepare,
        [((16, nodes), jnp.int32), ((4, 16, nodes), F32), own, ((16, LANES), jnp.int32)],
        stencil_index, stencil_coef, diag_margin, send_index,
    )
    ghost = exchange(ghost)
    rn, solved, *blocks = call(first_solve, [own, own] + block, partial, *ghost, send16, dinv)
    for _ in range(SWEEPS - 1):
        blocks = exchange(blocks)
        solved, *blocks = call(
            sweep, [own] + block, solved, *blocks, idx16, coef16, rn, dinv, send16
        )
    blocks = exchange(blocks)
    (out,) = call(
        edge_values,
        [((residual.shape[0] // LANES, LANES), F32)],
        solved, *blocks, tile(residual), tile(edge_scale), tangent, tile(edge_tail), tile(edge_head),
    )
    return out.reshape(-1)


def solution(mesh):
    return jax.shard_map(
        body,
        mesh=mesh,
        in_specs=(
            P(("grp", "sub")),
            P(("grp", "sub")),
            P(None, ("grp", "sub")),
            P(("grp", "sub")),
            P(("grp", "sub")),
            P(None, ("grp", "sub")),
            P(None, None, ("grp", "sub")),
            P(None, ("grp", "sub")),
            P("grp", "sub", None),
        ),
        out_specs=P(("grp", "sub")),
        check_vma=False,
    )
```

```python
import jax
import jax.numpy as jnp
from jax import lax
from jax.experimental import pallas as pl
from jax.experimental.pallas import tpu as pltpu
from jax.sharding import PartitionSpec as P


SWEEPS = 4
LANES = 128
F32 = jnp.float32
BF16 = jnp.bfloat16
VMEM = pl.BlockSpec(memory_space=pltpu.VMEM)
HBM = pl.BlockSpec(memory_space=pltpu.HBM)


def call(kernel, outs, *args, space=VMEM, scratch=()):
    return pl.pallas_call(
        kernel,
        out_shape=[jax.ShapeDtypeStruct(shape, dtype) for shape, dtype in outs],
        in_specs=[space] * len(args),
        out_specs=[VMEM] * len(outs),
        scratch_shapes=list(scratch),
        compiler_params=pltpu.CompilerParams(vmem_limit_bytes=16 << 20),
    )(*args)


def pairs(size, offset):
    route = []
    for k in range(size // 2):
        low, high = (2 * k + offset) % size, (2 * k + 1 + offset) % size
        route += [(low, high), (high, low)]
    return route


def split3(value):
    first = value.astype(BF16).astype(F32)
    rest = value - first
    second = rest.astype(BF16).astype(F32)
    third = (rest - second).astype(BF16).astype(F32)
    return (first, second, third)


def nt_dot(left, right):
    return lax.dot_general(left, right, (((1,), (1,)), ((), ())), preferred_element_type=F32)


def lane_pick(row, lane):
    wide = jnp.broadcast_to(row, lane.shape)
    return jnp.take_along_axis(wide, lane, axis=1, mode="promise_in_bounds")


def rows_of(index):
    return lax.shift_right_logical(index, 7), jnp.bitwise_and(index, LANES - 1)


def onehot(lane):
    n = lane.shape[1]
    iota = lax.broadcasted_iota(jnp.int32, (LANES, n), 0)
    return jnp.where(iota == lane, 1.0, 0.0).astype(BF16)


def masked(values, row, count):
    iota = lax.broadcasted_iota(jnp.int32, (count, row.shape[1]), 0)
    mask = iota == row
    return jnp.concatenate([jnp.where(mask, v, 0.0) for v in values], axis=0).astype(BF16)


def odd(axis):
    return jnp.bitwise_and(lax.axis_index(axis), 1)


def sides(parity, by_odd, by_even):
    low = jnp.where(parity == 1, by_even, by_odd)
    high = jnp.where(parity == 1, by_odd, by_even)
    return low, high


def edge_sums(res_hbm, tan_hbm, tail_hbm, head_hbm, own_ref, og_ref, eg_ref, os_ref, es_ref, res_ref, tan_ref, tail_ref, head_ref, sems):
    loads = [(res_hbm, res_ref), (tan_hbm, tan_ref), (tail_hbm, tail_ref), (head_hbm, head_ref)]
    loads = [pltpu.make_async_copy(src, dst, sems.at[i]) for i, (src, dst) in enumerate(loads)]
    for load in loads:
        load.start()
    for load in loads:
        load.wait()
    edges = res_ref.shape[1]
    chunk = 512
    total_head, total_tail = None, None
    for start in range(0, edges, chunk):
        cut = slice(start, start + chunk)
        res = res_ref[:, cut]
        half = [0.5 * tan_ref[c : c + 1, cut] * res for c in range(3)]
        head_row, head_lane = rows_of(head_ref[:, cut])
        head_row = jnp.where(head_row >= 4, head_row + 4, head_row)
        tail_row, tail_lane = rows_of(tail_ref[:, cut])
        parts = [split3(v) for v in [res] + half]
        parts = [parts[c][p] for p in range(3) for c in range(4)]
        signed = [-v if i % 4 == 0 else v for i, v in enumerate(parts)]
        by_head = nt_dot(masked(parts, head_row, 40), onehot(head_lane))
        by_tail = nt_dot(masked(signed, tail_row, 8), onehot(tail_lane))
        total_head = by_head if total_head is None else total_head + by_head
        total_tail = by_tail if total_tail is None else total_tail + by_tail
    g_odd, s_odd = odd("grp"), odd("sub")
    for c in range(4):
        head = total_head[40 * c : 40 * c + 40]
        tail = total_tail[8 * c : 8 * c + 8]
        for p in (1, 2):
            at = 4 * p + c
            head = head + total_head[40 * at : 40 * at + 40]
            tail = tail + total_tail[8 * at : 8 * at + 8]
        own_ref[4 * c : 4 * c + 4, :] = head[0:4] + tail[0:4]
        before, after, prev, nxt = (head[8 * i : 8 * i + 8] for i in range(1, 5))
        og_ref[c] = jnp.where(g_odd == 1, after, before)
        eg_ref[c] = jnp.where(g_odd == 1, before, after)
        os_ref[c] = jnp.where(s_odd == 1, nxt, prev)
        es_ref[c] = jnp.where(s_odd == 1, prev, nxt)


def prepare(idx_ref, coef_ref, margin_ref, send_ref, idx56_ref, coef56_ref, dinv_ref, send16_ref, wide_ref):
    count = idx_ref.shape[0]
    for j in range(count):
        for q in range(4):
            idx56_ref[4 * j + q : 4 * j + q + 1, :] = idx_ref[j : j + 1, LANES * q : LANES * q + LANES]
    for k in range(4):
        wide = coef_ref[k].astype(F32)
        wide_ref[k] = wide
        diag = (1.0 + margin_ref[k : k + 1, :]) * jnp.sum(jnp.abs(wide), axis=0, keepdims=True)
        inverse = 1.0 / diag
        for q in range(4):
            cols = slice(LANES * q, LANES * q + LANES)
            dinv_ref[4 * k + q : 4 * k + q + 1, :] = inverse[:, cols]
            for j in range(count):
                coef56_ref[k, 4 * j + q : 4 * j + q + 1, :] = wide_ref[k, j : j + 1, cols]
    for a in range(2):
        for b in range(2):
            for q in range(4):
                at = 8 * a + 4 * b + q
                send16_ref[at : at + 1, :] = send_ref[a, b : b + 1, LANES * q : LANES * q + LANES]


def send_blocks(solved, send_ref, outs):
    g_odd, s_odd = odd("grp"), odd("sub")
    og_ref, eg_ref, os_ref, es_ref = outs
    row, lane = rows_of(send_ref[...])
    for k in range(4):
        low, high = None, None
        got = []
        for half in range(2):
            part = slice(8 * half, 8 * half + 8)
            acc = lane_pick(solved[4 * k : 4 * k + 1], lane[part])
            for r in range(1, 4):
                acc = jnp.where(row[part] == r, lane_pick(solved[4 * k + r : 4 * k + r + 1], lane[part]), acc)
            got.append(acc)
        low, high = got
        og_ref[k] = jnp.where(g_odd == 1, high, low)
        eg_ref[k] = jnp.where(g_odd == 1, low, high)
        left = jnp.concatenate([low[0:4], high[0:4]], axis=0)
        right = jnp.concatenate([low[4:8], high[4:8]], axis=0)
        os_ref[k] = jnp.where(s_odd == 1, right, left)
        es_ref[k] = jnp.where(s_odd == 1, left, right)


def first_solve(own_ref, og, eg, os, es, send_ref, dinv_ref, rn_ref, y_ref, *outs):
    index = send_ref[...]
    row, lane = rows_of(index)
    lefts, rights = [], []
    values = []
    for c in range(4):
        before, after = sides(odd("grp"), og[c], eg[c])
        prev, nxt = sides(odd("sub"), os[c], es[c])
        low = before + jnp.concatenate([prev[0:4], nxt[0:4]], axis=0)
        high = after + jnp.concatenate([prev[4:8], nxt[4:8]], axis=0)
        values.append([split3(low), split3(high)])
    for half in range(2):
        for i in range(8):
            at = 8 * half + i
            cut = [values[c][half][p][i : i + 1] for p in range(3) for c in range(4)]
            lefts.append(masked(cut, row[at : at + 1], 8))
            rights.append(onehot(lane[at : at + 1]))
    total = nt_dot(jnp.concatenate(lefts, axis=1), jnp.concatenate(rights, axis=1))
    rows = []
    for c in range(4):
        rows.append(sum(total[8 * (4 * p + c) : 8 * (4 * p + c) + 4] for p in range(3)))
    rn = own_ref[...] + jnp.concatenate(rows, axis=0)
    solved = rn * dinv_ref[...]
    rn_ref[...] = rn
    y_ref[...] = solved
    send_blocks(solved, send_ref, outs)


def base_row(axis, matching):
    lower = {"grp": 4, "sub": 20}[axis]
    from_lower = odd(axis) != matching
    return jnp.where(from_lower, lower, lower + 8)


def block(axis, matching, ref):
    return base_row(axis, matching), [ref[k] for k in range(4)]


def early_blocks(y_ref, og_ref, os_ref):
    own = (0, [y_ref[4 * k : 4 * k + 4, :] for k in range(4)])
    return [own, block("grp", 1, og_ref), block("sub", 1, os_ref)]


def last_blocks(eg_ref, es_ref):
    return [block("grp", 0, eg_ref), block("sub", 0, es_ref)]


def gathered(blocks, index):
    rows, lanes = zip(*(rows_of(i) for i in index))
    acc = [[jnp.zeros(i.shape, F32)] * 4 for i in index]
    for v in range(len(index)):
        for base, table in blocks:
            for r in range(table[0].shape[0]):
                mask = rows[v] == base + r
                for k in range(4):
                    acc[v][k] = jnp.where(mask, lane_pick(table[k][r : r + 1], lanes[v]), acc[v][k])
    return acc


def vectors(ref):
    return [ref[8 * v : 8 * v + 8, :] for v in range(ref.shape[0] // 8)]


def stencil_sums(blocks, idx_ref, coef_ref):
    got = gathered(blocks, vectors(idx_ref))
    return [sum(got[v][k] * coef_ref[k, 8 * v : 8 * v + 8, :] for v in range(len(got))) for k in range(4)]


def sweep_early(y_ref, og_ref, os_ref, idx_ref, coef_ref, part_ref):
    for k, total in enumerate(stencil_sums(early_blocks(y_ref, og_ref, os_ref), idx_ref, coef_ref)):
        part_ref[8 * k : 8 * k + 8, :] = total


def sweep_last(eg_ref, es_ref, part_ref, idx_ref, coef_ref, rn_ref, dinv_ref, send_ref, new_ref, *outs):
    rows = []
    for k, total in enumerate(stencil_sums(last_blocks(eg_ref, es_ref), idx_ref, coef_ref)):
        total = total + part_ref[8 * k : 8 * k + 8, :]
        rows.append(total[0:4] + total[4:8])
    solved = (rn_ref[...] - jnp.concatenate(rows, axis=0)) * dinv_ref[...]
    new_ref[...] = solved
    send_blocks(solved, send_ref, outs)


def edge_early(y_ref, og_ref, os_ref, res_ref, scale_ref, tan_ref, tail_ref, head_ref, part_ref, tan24_ref):
    blocks = early_blocks(y_ref, og_ref, os_ref)
    heads = gathered(blocks, vectors(head_ref))
    tails = gathered(blocks[:1], vectors(tail_ref))
    for v in range(len(heads)):
        part = slice(8 * v, 8 * v + 8)
        mixed = None
        for c in range(3):
            pieces = [tan_ref[c : c + 1, LANES * i : LANES * i + LANES] for i in range(8 * v, 8 * v + 8)]
            tangent = jnp.concatenate(pieces, axis=0)
            tan24_ref[c, part, :] = tangent
            term = tangent * (tails[v][c + 1] + heads[v][c + 1])
            mixed = term if mixed is None else mixed + term
        part_ref[part, :] = scale_ref[part, :] * res_ref[part, :] + (heads[v][0] - tails[v][0]) + 0.5 * mixed


def edge_last(eg_ref, es_ref, part_ref, tan24_ref, head_ref, out_ref):
    heads = gathered(last_blocks(eg_ref, es_ref), vectors(head_ref))
    for v in range(len(heads)):
        part = slice(8 * v, 8 * v + 8)
        mixed = sum(tan24_ref[c, part, :] * heads[v][c + 1] for c in range(3))
        out_ref[part, :] = part_ref[part, :] + heads[v][0] + 0.5 * mixed


def exchange(blocks):
    og, eg, os, es = blocks
    grp, sub = lax.axis_size("grp"), lax.axis_size("sub")
    og = lax.ppermute(og, "grp", pairs(grp, 1))
    eg = lax.ppermute(eg, "grp", pairs(grp, 0))
    os = lax.ppermute(os, "sub", pairs(sub, 1))
    es = lax.ppermute(es, "sub", pairs(sub, 0))
    return og, eg, os, es


def body(
    residual,
    edge_scale,
    tangent,
    edge_tail,
    edge_head,
    stencil_index,
    stencil_coef,
    diag_margin,
    send_index,
):
    nodes = diag_margin.shape[1]
    own = ((16, LANES), F32)
    blocks4 = [((4, 8, LANES), F32)] * 4
    flat = lambda x: x.reshape(1, -1)
    tile = lambda x: x.reshape(-1, LANES)

    edges = residual.shape[0]
    wide_edges = [(1, edges), (3, edges), (1, edges), (1, edges)]
    types = [F32, F32, jnp.int32, jnp.int32]
    partial, *ghost = call(
        edge_sums,
        [own] + blocks4,
        *[pltpu.with_memory_space_constraint(x, pltpu.HBM) for x in (flat(residual), tangent, flat(edge_tail), flat(edge_head))],
        space=HBM,
        scratch=[pltpu.VMEM(shape, dtype) for shape, dtype in zip(wide_edges, types)] + [pltpu.SemaphoreType.DMA((4,))],
    )
    count = stencil_index.shape[0]
    lines = count * nodes // LANES
    ghost = exchange(ghost)
    idx56, coef56, dinv, send16 = call(
        prepare,
        [((lines, LANES), jnp.int32), ((4, lines, LANES), F32), own, ((16, LANES), jnp.int32)],
        stencil_index, stencil_coef, diag_margin, send_index,
        scratch=[pltpu.VMEM((4, count, nodes), F32)],
    )
    rn, solved, *blocks = call(first_solve, [own, own] + blocks4, partial, *ghost, send16, dinv)
    for _ in range(SWEEPS - 1):
        og, eg, os, es = exchange(blocks)
        (part,) = call(sweep_early, [((32, LANES), F32)], solved, og, os, idx56, coef56)
        solved, *blocks = call(sweep_last, [own] + blocks4, eg, es, part, idx56, coef56, rn, dinv, send16)
    on_edges = (edges // LANES, LANES)
    og, eg, os, es = exchange(blocks)
    part, tan24 = call(
        edge_early,
        [(on_edges, F32), ((3,) + on_edges, F32)],
        solved, og, os, tile(residual), tile(edge_scale), tangent, tile(edge_tail), tile(edge_head),
    )
    (out,) = call(edge_last, [(on_edges, F32)], eg, es, part, tan24, tile(edge_head))
    return out.reshape(-1)


def plain(mesh):
    return jax.shard_map(
        body,
        mesh=mesh,
        in_specs=(
            P(("grp", "sub")),
            P(("grp", "sub")),
            P(None, ("grp", "sub")),
            P(("grp", "sub")),
            P(("grp", "sub")),
            P(None, ("grp", "sub")),
            P(None, None, ("grp", "sub")),
            P(None, ("grp", "sub")),
            P("grp", "sub", None),
        ),
        out_specs=P(("grp", "sub")),
        check_vma=False,
    )


def solution(mesh):
    return plain(mesh)
```

```python
import jax
import jax.numpy as jnp
from jax import lax
from jax.experimental import pallas as pl
from jax.experimental.pallas import tpu as pltpu
from jax.sharding import PartitionSpec as P


SWEEPS = 4
LANES = 128
F32 = jnp.float32
BF16 = jnp.bfloat16
VMEM = pl.BlockSpec(memory_space=pltpu.VMEM)
HBM = pl.BlockSpec(memory_space=pltpu.HBM)


def call(kernel, outs, *args, space=VMEM, scratch=()):
    return pl.pallas_call(
        kernel,
        out_shape=[jax.ShapeDtypeStruct(shape, dtype) for shape, dtype in outs],
        in_specs=[space] * len(args),
        out_specs=[VMEM] * len(outs),
        scratch_shapes=list(scratch),
        compiler_params=pltpu.CompilerParams(vmem_limit_bytes=16 << 20),
    )(*args)


def pairs(size, offset):
    route = []
    for k in range(size // 2):
        low, high = (2 * k + offset) % size, (2 * k + 1 + offset) % size
        route += [(low, high), (high, low)]
    return route


def split3(value):
    first = value.astype(BF16).astype(F32)
    rest = value - first
    second = rest.astype(BF16).astype(F32)
    third = (rest - second).astype(BF16).astype(F32)
    return (first, second, third)


def nt_dot(left, right):
    return lax.dot_general(left, right, (((1,), (1,)), ((), ())), preferred_element_type=F32)


def lane_pick(row, lane):
    wide = jnp.broadcast_to(row, lane.shape)
    return jnp.take_along_axis(wide, lane, axis=1, mode="promise_in_bounds")


def rows_of(index):
    return lax.shift_right_logical(index, 7), jnp.bitwise_and(index, LANES - 1)


def onehot(lane):
    n = lane.shape[1]
    iota = lax.broadcasted_iota(jnp.int32, (LANES, n), 0).astype(F32).astype(BF16)
    return jnp.where(iota == lane.astype(F32).astype(BF16), jnp.ones((), BF16), jnp.zeros((), BF16))


def masked(values, row, count):
    iota = lax.broadcasted_iota(jnp.int32, (count, row.shape[1]), 0)
    mask = iota == row
    return jnp.concatenate([jnp.where(mask, v, 0.0) for v in values], axis=0).astype(BF16)


def odd(axis):
    return jnp.bitwise_and(lax.axis_index(axis), 1)


def sides(parity, by_odd, by_even):
    low = jnp.where(parity == 1, by_even, by_odd)
    high = jnp.where(parity == 1, by_odd, by_even)
    return low, high


def edge_parts(res_ref, tan_ref, cut):
    res = res_ref[:, cut]
    half = [0.5 * tan_ref[c : c + 1, cut] * res for c in range(3)]
    parts = [split3(v) for v in [res] + half]
    return [parts[c][p] for p in range(3) for c in range(4)]


def added(total, value):
    return value if total is None else total + value


def ghost_sums(
    res_hbm, tan_hbm, head_hbm, send_hbm, og_ref, eg_ref, os_ref, es_ref, res_ref, tan_ref, head_ref, send_ref, sems
):
    loads = [(res_hbm, res_ref), (tan_hbm, tan_ref), (head_hbm, head_ref), (send_hbm, send_ref)]
    loads = [pltpu.make_async_copy(src, dst, sems.at[i]) for i, (src, dst) in enumerate(loads)]
    for load in loads:
        load.start()
    for load in loads:
        load.wait()
    edges = res_ref.shape[1]
    chunk = edges // 2
    total = None
    for start in range(0, edges, chunk):
        cut = slice(start, start + chunk)
        row, lane = rows_of(head_ref[:, cut])
        total = added(total, nt_dot(masked(edge_parts(res_ref, tan_ref, cut), row - 4, 32), onehot(lane)))
    g_odd, s_odd = odd("grp"), odd("sub")
    for c in range(4):
        ghost = sum(total[32 * (4 * p + c) : 32 * (4 * p + c) + 32] for p in range(3))
        before, after, prev, nxt = (ghost[8 * i : 8 * i + 8] for i in range(4))
        og_ref[c] = jnp.where(g_odd == 1, after, before)
        eg_ref[c] = jnp.where(g_odd == 1, before, after)
        os_ref[c] = jnp.where(s_odd == 1, nxt, prev)
        es_ref[c] = jnp.where(s_odd == 1, prev, nxt)
    lists = [
        [[send_ref[a, b : b + 1, LANES * q : LANES * q + LANES] for q in range(4)] for b in range(2)] for a in range(2)
    ]
    joined = lambda first, second: jnp.concatenate(first + second, axis=0).astype(F32)
    low, high = joined(lists[0][0], lists[0][1]), joined(lists[1][0], lists[1][1])
    left, right = joined(lists[0][0], lists[1][0]), joined(lists[0][1], lists[1][1])
    og_ref[4] = jnp.where(g_odd == 1, high, low)
    eg_ref[4] = jnp.where(g_odd == 1, low, high)
    os_ref[4] = jnp.where(s_odd == 1, right, left)
    es_ref[4] = jnp.where(s_odd == 1, left, right)


def own_sums(res_ref, tan_ref, tail_ref, head_ref, own_ref):
    edges = res_ref.shape[1]
    chunk = edges // 2
    total = None
    for start in range(0, edges, chunk):
        cut = slice(start, start + chunk)
        parts = edge_parts(res_ref, tan_ref, cut)
        signed = [-v if i % 4 == 0 else v for i, v in enumerate(parts)]
        for values, index in ((parts, head_ref), (signed, tail_ref)):
            row, lane = rows_of(index[:, cut])
            total = added(total, nt_dot(masked(values, row, 8), onehot(lane)))
    for c in range(4):
        own_ref[4 * c : 4 * c + 4, :] = sum(total[8 * (4 * p + c) : 8 * (4 * p + c) + 4] for p in range(3))


def prepare(idx_ref, coef_ref, margin_ref, send_ref, idx56_ref, coef56_ref, dinv_ref, send16_ref, wide_ref):
    count = idx_ref.shape[0]
    for j in range(count):
        for q in range(4):
            idx56_ref[4 * j + q : 4 * j + q + 1, :] = idx_ref[j : j + 1, LANES * q : LANES * q + LANES]
    for k in range(4):
        wide = coef_ref[k].astype(F32)
        wide_ref[k] = wide
        diag = (1.0 + margin_ref[k : k + 1, :]) * jnp.sum(jnp.abs(wide), axis=0, keepdims=True)
        inverse = 1.0 / diag
        for q in range(4):
            cols = slice(LANES * q, LANES * q + LANES)
            dinv_ref[4 * k + q : 4 * k + q + 1, :] = inverse[:, cols]
            for j in range(count):
                coef56_ref[k, 4 * j + q : 4 * j + q + 1, :] = wide_ref[k, j : j + 1, cols]
    for a in range(2):
        for b in range(2):
            for q in range(4):
                at = 8 * a + 4 * b + q
                send16_ref[at : at + 1, :] = send_ref[a, b : b + 1, LANES * q : LANES * q + LANES]


def first_solve(own_ref, og, eg, os, es, send_ref, dinv_ref, rn_ref, y_ref):
    index = send_ref[...]
    row, lane = rows_of(index)
    lefts, rights = [], []
    values = []
    for c in range(4):
        before, after = sides(odd("grp"), og[c], eg[c])
        prev, nxt = sides(odd("sub"), os[c], es[c])
        low = before + jnp.concatenate([prev[0:4], nxt[0:4]], axis=0)
        high = after + jnp.concatenate([prev[4:8], nxt[4:8]], axis=0)
        values.append([split3(low), split3(high)])
    for half in range(2):
        for i in range(8):
            at = 8 * half + i
            cut = [values[c][half][p][i : i + 1] for p in range(3) for c in range(4)]
            lefts.append(masked(cut, row[at : at + 1], 8))
            rights.append(onehot(lane[at : at + 1]))
    total = nt_dot(jnp.concatenate(lefts, axis=1), jnp.concatenate(rights, axis=1))
    rows = []
    for c in range(4):
        rows.append(sum(total[8 * (4 * p + c) : 8 * (4 * p + c) + 4] for p in range(3)))
    rn = own_ref[...] + jnp.concatenate(rows, axis=0)
    rn_ref[...] = rn
    y_ref[...] = rn * dinv_ref[...]


def from_lower(axis, matching):
    return odd(axis) != matching


def compose(og_ref, eg_ref, os_ref, es_ref, idx_ref, head_ref, idx_out, head_out):
    blocks = []
    for axis, matching, ref, number in (("grp", 1, og_ref, 0), ("grp", 0, eg_ref, 0), ("sub", 1, os_ref, 2), ("sub", 0, es_ref, 2)):
        number = jnp.where(from_lower(axis, matching), number, number + 1)
        values = ref[4].astype(jnp.int32) + 4 * LANES * (number + 1)
        blocks.append((4 + 8 * number, values.astype(F32)))
    for src, dst in ((idx_ref, idx_out), (head_ref, head_out)):
        for v, index in enumerate(vectors(src)):
            row, lane = rows_of(index)
            acc = index.astype(F32)
            for base, values in blocks:
                for r in range(8):
                    acc = jnp.where(row == base + r, lane_pick(values[r : r + 1], lane), acc)
            dst[8 * v : 8 * v + 8, :] = acc.astype(jnp.int32)


def block(axis, matching, ref):
    lower = {"grp": 4, "sub": 12}[axis]
    base = jnp.where(from_lower(axis, matching), lower, lower + 4)
    return base, [ref[4 * k : 4 * k + 4, :] for k in range(4)]


def early_blocks(y_ref, og_ref, os_ref):
    own = (0, [y_ref[4 * k : 4 * k + 4, :] for k in range(4)])
    return [own, block("grp", 1, og_ref), block("sub", 1, os_ref)]


def last_blocks(eg_ref, es_ref):
    return [block("grp", 0, eg_ref), block("sub", 0, es_ref)]


def gathered(blocks, index):
    rows, lanes = zip(*(rows_of(i) for i in index))
    acc = [[jnp.zeros(i.shape, F32)] * 4 for i in index]
    for v in range(len(index)):
        for base, table in blocks:
            for r in range(table[0].shape[0]):
                mask = rows[v] == base + r
                for k in range(4):
                    acc[v][k] = jnp.where(mask, lane_pick(table[k][r : r + 1], lanes[v]), acc[v][k])
    return acc


def vectors(ref):
    return [ref[8 * v : 8 * v + 8, :] for v in range(ref.shape[0] // 8)]


def stencil_sums(blocks, idx_ref, coef_ref):
    got = gathered(blocks, vectors(idx_ref))
    return [sum(got[v][k] * coef_ref[k, 8 * v : 8 * v + 8, :] for v in range(len(got))) for k in range(4)]


def sweep_early(y_ref, og_ref, os_ref, idx_ref, coef_ref, part_ref):
    for k, total in enumerate(stencil_sums(early_blocks(y_ref, og_ref, os_ref), idx_ref, coef_ref)):
        part_ref[8 * k : 8 * k + 8, :] = total


def sweep_last(eg_ref, es_ref, part_ref, idx_ref, coef_ref, rn_ref, dinv_ref, new_ref):
    rows = []
    for k, total in enumerate(stencil_sums(last_blocks(eg_ref, es_ref), idx_ref, coef_ref)):
        total = total + part_ref[8 * k : 8 * k + 8, :]
        rows.append(total[0:4] + total[4:8])
    new_ref[...] = (rn_ref[...] - jnp.concatenate(rows, axis=0)) * dinv_ref[...]


def edge_early(y_ref, og_ref, os_ref, res_ref, scale_ref, tan_ref, tail_ref, head_ref, part_ref, tan24_ref):
    blocks = early_blocks(y_ref, og_ref, os_ref)
    heads = gathered(blocks, vectors(head_ref))
    tails = gathered(blocks[:1], vectors(tail_ref))
    for v in range(len(heads)):
        part = slice(8 * v, 8 * v + 8)
        mixed = None
        for c in range(3):
            pieces = [tan_ref[c : c + 1, LANES * i : LANES * i + LANES] for i in range(8 * v, 8 * v + 8)]
            tangent = jnp.concatenate(pieces, axis=0)
            tan24_ref[c, part, :] = tangent
            term = tangent * (tails[v][c + 1] + heads[v][c + 1])
            mixed = term if mixed is None else mixed + term
        part_ref[part, :] = scale_ref[part, :] * res_ref[part, :] + (heads[v][0] - tails[v][0]) + 0.5 * mixed


def edge_last(eg_ref, es_ref, part_ref, tan24_ref, head_ref, out_ref):
    heads = gathered(last_blocks(eg_ref, es_ref), vectors(head_ref))
    for v in range(len(heads)):
        part = slice(8 * v, 8 * v + 8)
        mixed = sum(tan24_ref[c, part, :] * heads[v][c + 1] for c in range(3))
        out_ref[part, :] = part_ref[part, :] + heads[v][0] + 0.5 * mixed


def exchange(blocks):
    og, eg, os, es = blocks
    grp, sub = lax.axis_size("grp"), lax.axis_size("sub")
    og = lax.ppermute(og, "grp", pairs(grp, 1))
    eg = lax.ppermute(eg, "grp", pairs(grp, 0))
    os = lax.ppermute(os, "sub", pairs(sub, 1))
    es = lax.ppermute(es, "sub", pairs(sub, 0))
    return og, eg, os, es


def body(
    residual,
    edge_scale,
    tangent,
    edge_tail,
    edge_head,
    stencil_index,
    stencil_coef,
    diag_margin,
    send_index,
):
    nodes = diag_margin.shape[1]
    own = ((16, LANES), F32)
    blocks4 = [((5, 8, LANES), F32)] * 4
    flat = lambda x: x.reshape(1, -1)
    tile = lambda x: x.reshape(-1, LANES)

    edges = residual.shape[0]
    on_hbm = lambda x: pltpu.with_memory_space_constraint(x, pltpu.HBM)
    loaded = [((1, edges), F32), ((3, edges), F32), ((1, edges), jnp.int32), (send_index.shape, jnp.int32)]
    ghost = call(
        ghost_sums,
        blocks4,
        on_hbm(flat(residual)), on_hbm(tangent), on_hbm(flat(edge_head)), on_hbm(send_index),
        space=HBM,
        scratch=[pltpu.VMEM(shape, dtype) for shape, dtype in loaded] + [pltpu.SemaphoreType.DMA((4,))],
    )
    count = stencil_index.shape[0]
    lines = count * nodes // LANES
    ghost = exchange(ghost)
    idx56, coef56, dinv, send16 = call(
        prepare,
        [((lines, LANES), jnp.int32), ((4, lines, LANES), F32), own, ((16, LANES), jnp.int32)],
        stencil_index, stencil_coef, diag_margin, send_index,
        scratch=[pltpu.VMEM((4, count, nodes), F32)],
    )
    (partial,) = call(own_sums, [own], flat(residual), tangent, flat(edge_tail), flat(edge_head))
    rn, solved = call(first_solve, [own, own], partial, *ghost, send16, dinv)
    on_edges = (edges // LANES, LANES)
    for step in range(SWEEPS - 1):
        og, eg, os, es = exchange([solved] * 4)
        if step == 0:
            idx56, head24 = call(
                compose, [((lines, LANES), jnp.int32), (on_edges, jnp.int32)], *ghost, idx56, tile(edge_head)
            )
        (part,) = call(sweep_early, [((32, LANES), F32)], solved, og, os, idx56, coef56)
        (solved,) = call(sweep_last, [own], eg, es, part, idx56, coef56, rn, dinv)
    og, eg, os, es = exchange([solved] * 4)
    part, tan24 = call(
        edge_early,
        [(on_edges, F32), ((3,) + on_edges, F32)],
        solved, og, os, tile(residual), tile(edge_scale), tangent, tile(edge_tail), head24,
    )
    (out,) = call(edge_last, [(on_edges, F32)], eg, es, part, tan24, head24)
    return out.reshape(-1)


def plain(mesh):
    return jax.shard_map(
        body,
        mesh=mesh,
        in_specs=(
            P(("grp", "sub")),
            P(("grp", "sub")),
            P(None, ("grp", "sub")),
            P(("grp", "sub")),
            P(("grp", "sub")),
            P(None, ("grp", "sub")),
            P(None, None, ("grp", "sub")),
            P(None, ("grp", "sub")),
            P("grp", "sub", None),
        ),
        out_specs=P(("grp", "sub")),
        check_vma=False,
    )


def solution(mesh):
    return plain(mesh)
```

```python
import jax
import jax.numpy as jnp
from jax import lax
from jax.experimental import pallas as pl
from jax.experimental.pallas import tpu as pltpu
from jax.sharding import PartitionSpec as P


SWEEPS = 4
EARLY_ROW = 12
LANES = 128
F32 = jnp.float32
BF16 = jnp.bfloat16
VMEM = pl.BlockSpec(memory_space=pltpu.VMEM)
HBM = pl.BlockSpec(memory_space=pltpu.HBM)


def call(kernel, outs, *args, space=VMEM, scratch=()):
    return pl.pallas_call(
        kernel,
        out_shape=[jax.ShapeDtypeStruct(shape, dtype) for shape, dtype in outs],
        in_specs=[space] * len(args),
        out_specs=[VMEM] * len(outs),
        scratch_shapes=list(scratch),
        compiler_params=pltpu.CompilerParams(vmem_limit_bytes=16 << 20),
    )(*args)


def pairs(size, offset):
    route = []
    for k in range(size // 2):
        low, high = (2 * k + offset) % size, (2 * k + 1 + offset) % size
        route += [(low, high), (high, low)]
    return route


def split3(value):
    first = value.astype(BF16).astype(F32)
    rest = value - first
    second = rest.astype(BF16).astype(F32)
    third = (rest - second).astype(BF16).astype(F32)
    return (first, second, third)


def nt_dot(left, right):
    return lax.dot_general(left, right, (((1,), (1,)), ((), ())), preferred_element_type=F32)


def lane_pick(row, lane):
    wide = jnp.broadcast_to(row, lane.shape)
    return jnp.take_along_axis(wide, lane, axis=1, mode="promise_in_bounds")


def rows_of(index):
    return lax.shift_right_logical(index, 7), jnp.bitwise_and(index, LANES - 1)


def onehot(lane):
    n = lane.shape[1]
    iota = lax.broadcasted_iota(jnp.int32, (LANES, n), 0).astype(F32).astype(BF16)
    return jnp.where(iota == lane.astype(F32).astype(BF16), jnp.ones((), BF16), jnp.zeros((), BF16))


def masked(values, row, count):
    iota = lax.broadcasted_iota(jnp.int32, (count, row.shape[1]), 0)
    mask = iota == row
    return jnp.concatenate([jnp.where(mask, v, 0.0) for v in values], axis=0).astype(BF16)


def odd(axis):
    return jnp.bitwise_and(lax.axis_index(axis), 1)


def sides(parity, by_odd, by_even):
    low = jnp.where(parity == 1, by_even, by_odd)
    high = jnp.where(parity == 1, by_odd, by_even)
    return low, high


def edge_parts(res_ref, tan_ref, cut):
    res = res_ref[:, cut]
    half = [0.5 * tan_ref[c : c + 1, cut] * res for c in range(3)]
    parts = [split3(v) for v in [res] + half]
    return [parts[c][p] for p in range(3) for c in range(4)]


def added(total, value):
    return value if total is None else total + value


def ghost_sums(
    res_hbm, tan_hbm, head_hbm, send_hbm, og_ref, eg_ref, os_ref, es_ref, res_ref, tan_ref, head_ref, send_ref, sems
):
    loads = [(res_hbm, res_ref), (tan_hbm, tan_ref), (head_hbm, head_ref), (send_hbm, send_ref)]
    loads = [pltpu.make_async_copy(src, dst, sems.at[i]) for i, (src, dst) in enumerate(loads)]
    for load in loads:
        load.start()
    for load in loads:
        load.wait()
    edges = res_ref.shape[1]
    chunk = edges // 2
    total = None
    for start in range(0, edges, chunk):
        cut = slice(start, start + chunk)
        row, lane = rows_of(head_ref[:, cut])
        total = added(total, nt_dot(masked(edge_parts(res_ref, tan_ref, cut), row - 4, 32), onehot(lane)))
    g_odd, s_odd = odd("grp"), odd("sub")
    for c in range(4):
        ghost = sum(total[32 * (4 * p + c) : 32 * (4 * p + c) + 32] for p in range(3))
        before, after, prev, nxt = (ghost[8 * i : 8 * i + 8] for i in range(4))
        og_ref[c] = jnp.where(g_odd == 1, after, before)
        eg_ref[c] = jnp.where(g_odd == 1, before, after)
        os_ref[c] = jnp.where(s_odd == 1, nxt, prev)
        es_ref[c] = jnp.where(s_odd == 1, prev, nxt)
    lists = [
        [[send_ref[a, b : b + 1, LANES * q : LANES * q + LANES] for q in range(4)] for b in range(2)] for a in range(2)
    ]
    joined = lambda first, second: jnp.concatenate(first + second, axis=0).astype(F32)
    low, high = joined(lists[0][0], lists[0][1]), joined(lists[1][0], lists[1][1])
    left, right = joined(lists[0][0], lists[1][0]), joined(lists[0][1], lists[1][1])
    og_ref[4] = jnp.where(g_odd == 1, high, low)
    eg_ref[4] = jnp.where(g_odd == 1, low, high)
    os_ref[4] = jnp.where(s_odd == 1, right, left)
    es_ref[4] = jnp.where(s_odd == 1, left, right)


def own_sums(res_ref, tan_ref, tail_ref, head_ref, own_ref):
    edges = res_ref.shape[1]
    chunk = edges // 2
    total = None
    for start in range(0, edges, chunk):
        cut = slice(start, start + chunk)
        parts = edge_parts(res_ref, tan_ref, cut)
        signed = [-v if i % 4 == 0 else v for i, v in enumerate(parts)]
        for values, index in ((parts, head_ref), (signed, tail_ref)):
            row, lane = rows_of(index[:, cut])
            total = added(total, nt_dot(masked(values, row, 8), onehot(lane)))
    for c in range(4):
        own_ref[4 * c : 4 * c + 4, :] = sum(total[8 * (4 * p + c) : 8 * (4 * p + c) + 4] for p in range(3))


def prepare(idx_ref, coef_ref, margin_ref, send_ref, idx56_ref, coef56_ref, dinv_ref, send16_ref, wide_ref):
    count = idx_ref.shape[0]
    for j in range(count):
        for q in range(4):
            idx56_ref[4 * j + q : 4 * j + q + 1, :] = idx_ref[j : j + 1, LANES * q : LANES * q + LANES]
    for k in range(4):
        wide = coef_ref[k].astype(F32)
        wide_ref[k] = wide
        diag = (1.0 + margin_ref[k : k + 1, :]) * jnp.sum(jnp.abs(wide), axis=0, keepdims=True)
        inverse = 1.0 / diag
        for q in range(4):
            cols = slice(LANES * q, LANES * q + LANES)
            dinv_ref[4 * k + q : 4 * k + q + 1, :] = inverse[:, cols]
            for j in range(count):
                coef56_ref[k, 4 * j + q : 4 * j + q + 1, :] = wide_ref[k, j : j + 1, cols]
    for a in range(2):
        for b in range(2):
            for q in range(4):
                at = 8 * a + 4 * b + q
                send16_ref[at : at + 1, :] = send_ref[a, b : b + 1, LANES * q : LANES * q + LANES]


def first_solve(own_ref, og, eg, os_early, os_late, es, send_ref, dinv_ref, rn_ref, y_ref):
    index = send_ref[...]
    row, lane = rows_of(index)
    lefts, rights = [], []
    values = []
    for c in range(4):
        before, after = sides(odd("grp"), og[c], eg[c])
        prev, nxt = sides(odd("sub"), os_early[c] + os_late[c], es[c])
        low = before + jnp.concatenate([prev[0:4], nxt[0:4]], axis=0)
        high = after + jnp.concatenate([prev[4:8], nxt[4:8]], axis=0)
        values.append([split3(low), split3(high)])
    for half in range(2):
        for i in range(8):
            at = 8 * half + i
            cut = [values[c][half][p][i : i + 1] for p in range(3) for c in range(4)]
            lefts.append(masked(cut, row[at : at + 1], 8))
            rights.append(onehot(lane[at : at + 1]))
    total = nt_dot(jnp.concatenate(lefts, axis=1), jnp.concatenate(rights, axis=1))
    rows = []
    for c in range(4):
        rows.append(sum(total[8 * (4 * p + c) : 8 * (4 * p + c) + 4] for p in range(3)))
    rn = own_ref[...] + jnp.concatenate(rows, axis=0)
    rn_ref[...] = rn
    y_ref[...] = rn * dinv_ref[...]


def from_lower(axis, matching):
    return odd(axis) != matching


def compose(og_ref, eg_ref, os_early_ref, os_late_ref, es_ref, idx_ref, head_ref, idx_out, head_out):
    blocks = []
    received = [og_ref[4], eg_ref[4], os_early_ref[4] + os_late_ref[4], es_ref[4]]
    for values, (axis, matching, number) in zip(received, (("grp", 1, 0), ("grp", 0, 0), ("sub", 1, 2), ("sub", 0, 2))):
        number = jnp.where(from_lower(axis, matching), number, number + 1)
        values = values.astype(jnp.int32) + 4 * LANES * (number + 1)
        blocks.append((4 + 8 * number, values.astype(F32)))
    for src, dst in ((idx_ref, idx_out), (head_ref, head_out)):
        for v, index in enumerate(vectors(src)):
            row, lane = rows_of(index)
            acc = index.astype(F32)
            for base, values in blocks:
                for r in range(8):
                    acc = jnp.where(row == base + r, lane_pick(values[r : r + 1], lane), acc)
            dst[8 * v : 8 * v + 8, :] = acc.astype(jnp.int32)


def block(axis, matching, ref):
    lower = {"grp": 4, "sub": 12}[axis]
    base = jnp.where(from_lower(axis, matching), lower, lower + 4)
    return base, [ref[4 * k : 4 * k + 4, :] for k in range(4)]


def early_blocks(y_ref, og_ref, os_ref):
    own = (0, [y_ref[4 * k : 4 * k + 4, :] for k in range(4)])
    return [own, block("grp", 1, og_ref), block("sub", 1, os_ref)]


def last_blocks(eg_ref, es_ref):
    return [block("grp", 0, eg_ref), block("sub", 0, es_ref)]


def gathered(blocks, index):
    rows, lanes = zip(*(rows_of(i) for i in index))
    acc = [[jnp.zeros(i.shape, F32)] * 4 for i in index]
    for v in range(len(index)):
        for base, table in blocks:
            for r in range(table[0].shape[0]):
                mask = rows[v] == base + r
                for k in range(4):
                    acc[v][k] = jnp.where(mask, lane_pick(table[k][r : r + 1], lanes[v]), acc[v][k])
    return acc


def vectors(ref):
    return [ref[8 * v : 8 * v + 8, :] for v in range(ref.shape[0] // 8)]


def stencil_sums(blocks, idx_ref, coef_ref):
    got = gathered(blocks, vectors(idx_ref))
    return [sum(got[v][k] * coef_ref[k, 8 * v : 8 * v + 8, :] for v in range(len(got))) for k in range(4)]


def sweep_early(y_ref, og_ref, os_ref, idx_ref, coef_ref, part_ref):
    for k, total in enumerate(stencil_sums(early_blocks(y_ref, og_ref, os_ref), idx_ref, coef_ref)):
        part_ref[8 * k : 8 * k + 8, :] = total


def sweep_last(eg_ref, es_ref, part_ref, idx_ref, coef_ref, rn_ref, dinv_ref, new_ref):
    rows = []
    for k, total in enumerate(stencil_sums(last_blocks(eg_ref, es_ref), idx_ref, coef_ref)):
        total = total + part_ref[8 * k : 8 * k + 8, :]
        rows.append(total[0:4] + total[4:8])
    new_ref[...] = (rn_ref[...] - jnp.concatenate(rows, axis=0)) * dinv_ref[...]


def edge_early(y_ref, og_ref, os_ref, res_ref, scale_ref, tan_ref, tail_ref, head_ref, part_ref, tan24_ref):
    blocks = early_blocks(y_ref, og_ref, os_ref)
    heads = gathered(blocks, vectors(head_ref))
    tails = gathered(blocks[:1], vectors(tail_ref))
    for v in range(len(heads)):
        part = slice(8 * v, 8 * v + 8)
        mixed = None
        for c in range(3):
            pieces = [tan_ref[c : c + 1, LANES * i : LANES * i + LANES] for i in range(8 * v, 8 * v + 8)]
            tangent = jnp.concatenate(pieces, axis=0)
            tan24_ref[c, part, :] = tangent
            term = tangent * (tails[v][c + 1] + heads[v][c + 1])
            mixed = term if mixed is None else mixed + term
        part_ref[part, :] = scale_ref[part, :] * res_ref[part, :] + (heads[v][0] - tails[v][0]) + 0.5 * mixed


def edge_last(eg_ref, es_ref, part_ref, tan24_ref, head_ref, out_ref):
    heads = gathered(last_blocks(eg_ref, es_ref), vectors(head_ref))
    for v in range(len(heads)):
        part = slice(8 * v, 8 * v + 8)
        mixed = sum(tan24_ref[c, part, :] * heads[v][c + 1] for c in range(3))
        out_ref[part, :] = part_ref[part, :] + heads[v][0] + 0.5 * mixed


def row_pairs(rows, size, offset):
    return [(size * row + a, size * row + b) for row in rows for a, b in pairs(size, offset)]


def first_exchange(blocks):
    og, eg, os, es = blocks
    grp, sub = lax.axis_size("grp"), lax.axis_size("sub")
    early = range(0, grp, EARLY_ROW)
    others = [row for row in range(grp) if row not in early]
    os_early = lax.ppermute(os, ("grp", "sub"), row_pairs(early, sub, 1))
    og = lax.ppermute(og, "grp", pairs(grp, 1))
    os_late = lax.ppermute(os, ("grp", "sub"), row_pairs(others, sub, 1))
    eg = lax.ppermute(eg, "grp", pairs(grp, 0))
    es = lax.ppermute(es, "sub", pairs(sub, 0))
    return og, eg, os_early, os_late, es


def exchange(blocks):
    og, eg, os, es = blocks
    grp, sub = lax.axis_size("grp"), lax.axis_size("sub")
    og = lax.ppermute(og, "grp", pairs(grp, 1))
    eg = lax.ppermute(eg, "grp", pairs(grp, 0))
    os = lax.ppermute(os, "sub", pairs(sub, 1))
    es = lax.ppermute(es, "sub", pairs(sub, 0))
    return og, eg, os, es


def body(
    residual,
    edge_scale,
    tangent,
    edge_tail,
    edge_head,
    stencil_index,
    stencil_coef,
    diag_margin,
    send_index,
):
    nodes = diag_margin.shape[1]
    own = ((16, LANES), F32)
    blocks4 = [((5, 8, LANES), F32)] * 4
    flat = lambda x: x.reshape(1, -1)
    tile = lambda x: x.reshape(-1, LANES)

    edges = residual.shape[0]
    on_hbm = lambda x: pltpu.with_memory_space_constraint(x, pltpu.HBM)
    loaded = [((1, edges), F32), ((3, edges), F32), ((1, edges), jnp.int32), (send_index.shape, jnp.int32)]
    ghost = call(
        ghost_sums,
        blocks4,
        on_hbm(flat(residual)), on_hbm(tangent), on_hbm(flat(edge_head)), on_hbm(send_index),
        space=HBM,
        scratch=[pltpu.VMEM(shape, dtype) for shape, dtype in loaded] + [pltpu.SemaphoreType.DMA((4,))],
    )
    count = stencil_index.shape[0]
    lines = count * nodes // LANES
    ghost = first_exchange(ghost)
    idx56, coef56, dinv, send16 = call(
        prepare,
        [((lines, LANES), jnp.int32), ((4, lines, LANES), F32), own, ((16, LANES), jnp.int32)],
        stencil_index, stencil_coef, diag_margin, send_index,
        scratch=[pltpu.VMEM((4, count, nodes), F32)],
    )
    (partial,) = call(own_sums, [own], flat(residual), tangent, flat(edge_tail), flat(edge_head))
    rn, solved = call(first_solve, [own, own], partial, *ghost, send16, dinv)
    on_edges = (edges // LANES, LANES)
    for step in range(SWEEPS - 1):
        og, eg, os, es = exchange([solved] * 4)
        if step == 0:
            idx56, head24 = call(
                compose, [((lines, LANES), jnp.int32), (on_edges, jnp.int32)], *ghost, idx56, tile(edge_head)
            )
        (part,) = call(sweep_early, [((32, LANES), F32)], solved, og, os, idx56, coef56)
        (solved,) = call(sweep_last, [own], eg, es, part, idx56, coef56, rn, dinv)
    og, eg, os, es = exchange([solved] * 4)
    part, tan24 = call(
        edge_early,
        [(on_edges, F32), ((3,) + on_edges, F32)],
        solved, og, os, tile(residual), tile(edge_scale), tangent, tile(edge_tail), head24,
    )
    (out,) = call(edge_last, [(on_edges, F32)], eg, es, part, tan24, head24)
    return out.reshape(-1)


def plain(mesh):
    return jax.shard_map(
        body,
        mesh=mesh,
        in_specs=(
            P(("grp", "sub")),
            P(("grp", "sub")),
            P(None, ("grp", "sub")),
            P(("grp", "sub")),
            P(("grp", "sub")),
            P(None, ("grp", "sub")),
            P(None, None, ("grp", "sub")),
            P(None, ("grp", "sub")),
            P("grp", "sub", None),
        ),
        out_specs=P(("grp", "sub")),
        check_vma=False,
    )


def solution(mesh):
    return plain(mesh)
```
